32 devices in a mesh: vox: 8 (over y, x, core), sen: 4 (over z).
Axes of the slice: x: 2, y: 2, z: 4, core: 2. Of those that a mesh axis runs over, the one named last changes fastest.
Arguments:
- image: float32 [8, 2, 512], P('vox'), may hold values from -6 to 6
- weights: bfloat16 [8, 4, 5, 1024, 1024], P('vox', 'sen'), may hold values from -0.0625 to 0.0625
- block_ids: int32 [8, 4, 5], P('vox', 'sen'), may hold values from 0 to 15
- offsets: int32 [8, 4, 5], P('vox', 'sen'), may hold values from 0 to 1984
- counts: int32 [8, 4], P('vox', 'sen'), may hold values from 1 to 5, as said below
- measured: bfloat16 [4, 256, 2048], P('sen', 'vox'), may hold values from -6 to 6
Outputs:
- image_next: float32 [8, 2, 512], P('vox')
- residual: float32 [4, 256, 2048], P('sen', 'vox')
The draws below stay inside these ranges and needn't reach their ends.
Inputs may be any that keep to these rules, and one draw needn't show every extreme that they name: `counts`: some slab and group has all 5 slots live in every draw.
All inputs are finite; a program needn't handle non-finite values.
Results may differ from the reference program's by a relative error of at most 0.0025.
Values may be sent and summed in bfloat16 or wider, within the bound.
A program may use at most 64 MiB of HBM per device.

```python
import jax
import jax.numpy as jnp
from jax import lax

SAMPLES = 2048
SB = 16
WIN = 64
K_MAX = 5
ZS = 1
PY = 2
PX = 512
SLABS = 8
GROUPS = 4
GSENS = 256
BLOCKS = 16
NZ = 8


def draw_counts(key, part):
    first_key, second_key = jax.random.split(jax.random.fold_in(key, 17))
    drawn_counts = jax.random.randint(first_key, (SLABS, GROUPS), 1, K_MAX + 1)
    chosen = jax.random.randint(second_key, (), 0, SLABS * GROUPS)
    flat_index = jnp.arange(SLABS * GROUPS).reshape(SLABS, GROUPS)
    return jnp.where(flat_index == chosen, K_MAX, drawn_counts).astype(jnp.int32)


def touch_ends(drawn, key, least, largest):
    shape = drawn.shape
    spot = [jax.random.randint(jax.random.fold_in(key, axis), (), 0, shape[axis]) for axis in range(len(shape))]
    drawn = drawn.at[tuple(spot)].set(least)
    longest = shape.index(max(shape))
    spot[longest] = (spot[longest] + 1) % shape[longest]
    return drawn.at[tuple(spot)].set(largest)


def steps_of(rng, extent, cuts, low, high):
    gain, own = 1.0, jax.random.fold_in(rng, 6)
    for dim, blocks in cuts:
        draws = jnp.exp(jax.random.uniform(jax.random.fold_in(own, dim), (blocks,), jnp.float32, low / len(cuts), high / len(cuts)))
        gain = gain * jnp.repeat(draws, extent[dim] // blocks).reshape([-1 if axis == dim else 1 for axis in range(len(extent))])
    return gain


def normal_values(rng, shape, width, limit, cuts=(), held_as=jnp.bfloat16):
    loudness = steps_of(rng, shape, cuts, -0.22, 0.18) if cuts else 1.0
    array = jax.random.normal(rng, shape, jnp.float32) * width * loudness
    return jnp.minimum(jnp.maximum(array, -limit), limit).astype(held_as)


def setup_inputs(seed: int = 0) -> dict:
    arg_keys = jax.random.split(jax.random.key(seed), 7)
    return {
        "image": normal_values(arg_keys[0], (NZ, PY, PX), 1.0, 6.0, ((0, 8),), jnp.float32),
        "weights": normal_values(arg_keys[1], (SLABS, GROUPS, K_MAX, ZS * PY * PX, SB * WIN), (8 * SB * WIN) ** -0.5, 0.0625, ((0, 8), (1, 4))),
        "block_ids": touch_ends(jax.random.randint(arg_keys[2], (SLABS, GROUPS, K_MAX), 0, BLOCKS), jax.random.fold_in(arg_keys[2], 1), 0, BLOCKS - 1).astype(jnp.int32),
        "offsets": touch_ends(jax.random.randint(arg_keys[3], (SLABS, GROUPS, K_MAX), 0, SAMPLES - WIN + 1), jax.random.fold_in(arg_keys[3], 1), 0, SAMPLES - WIN).astype(jnp.int32),
        "counts": draw_counts(jax.random.fold_in(arg_keys[6], 71), 0),
        "measured": normal_values(arg_keys[5], (GROUPS, GSENS, SAMPLES), 1.0, 6.0, ((0, 4), (1, 8))),
    }


TAPS = ((-2, 1.0 / 12.0), (-1, -8.0 / 12.0), (1, 8.0 / 12.0), (2, -1.0 / 12.0))
STEP_SIZE = 0.25
TV_WEIGHT = 0.3
TV_EPS = 0.01

def derivative(signal):
    length_t = signal.shape[-1]
    padded = jnp.pad(signal, [(0, 0)] * (signal.ndim - 1) + [(2, 2)])
    summed = jnp.zeros_like(signal)
    for shift_by, coefficient in TAPS:
        summed = summed + coefficient * padded[..., 2 + shift_by:2 + shift_by + length_t]
    return summed

def forward_step(volume, axis_dim):
    length_a = volume.shape[axis_dim]
    ahead = jnp.concatenate([lax.slice_in_dim(volume, 1, length_a, axis=axis_dim), lax.slice_in_dim(volume, length_a - 1, length_a, axis=axis_dim)], axis=axis_dim)
    return ahead - volume

def backward_shift(field, axis_dim):
    length_a = field.shape[axis_dim]
    zero_row = jnp.zeros_like(lax.slice_in_dim(field, 0, 1, axis=axis_dim))
    return jnp.concatenate([zero_row, lax.slice_in_dim(field, 0, length_a - 1, axis=axis_dim)], axis=axis_dim)

def tv_gradient(volume):
    step_z = forward_step(volume, 0)
    step_y = forward_step(volume, 1)
    step_x = forward_step(volume, 2)
    magnitude = jnp.sqrt(step_z * step_z + step_y * step_y + step_x * step_x + TV_EPS)
    result = jnp.zeros_like(volume)
    for axis_dim, step_a in ((0, step_z), (1, step_y), (2, step_x)):
        unit_a = step_a / magnitude
        result = result + backward_shift(unit_a, axis_dim) - unit_a
    return result

def reference(image, weights, block_ids, offsets, counts, measured):
    voxels = image.astype(jnp.bfloat16).astype(jnp.float32).reshape(SLABS, ZS * PY * PX)
    slot_grid = jnp.arange(K_MAX, dtype=jnp.int32)

    def add_slab(signals, inputs):
        slab_voxels, slab_blocks, slab_ids, slab_starts, slab_counts = inputs
        pieces = jnp.einsum('v,gkvc->gkc', slab_voxels, slab_blocks.astype(jnp.float32))

        def place(flat_index, acc):
            group_index = (flat_index // K_MAX).astype(jnp.int32)
            slot_index = (flat_index % K_MAX).astype(jnp.int32)
            live_flag = (slot_index < slab_counts[group_index]).astype(jnp.float32)
            piece = pieces[group_index, slot_index].reshape(1, SB, WIN) * live_flag
            corner = (group_index, (slab_ids[group_index, slot_index] * SB).astype(jnp.int32), slab_starts[group_index, slot_index].astype(jnp.int32))
            current = lax.dynamic_slice(acc, corner, (1, SB, WIN))
            return lax.dynamic_update_slice(acc, current + piece, corner)
        signals = lax.fori_loop(0, GROUPS * K_MAX, place, signals)
        return (signals, None)
    zero_signals = jnp.zeros((GROUPS, GSENS, SAMPLES), jnp.float32)
    signals, _ = lax.scan(add_slab, zero_signals, (voxels, weights, block_ids, offsets, counts))
    residual = derivative(signals) - measured.astype(jnp.float32)
    adjoint = lax.optimization_barrier((-derivative(residual)).astype(jnp.bfloat16)).astype(jnp.float32)
    group_grid = jnp.broadcast_to(jnp.arange(GROUPS, dtype=jnp.int32)[:, None], (GROUPS, K_MAX))

    def cut_window(group_index, block_index, start):
        corner = (group_index, (block_index * SB).astype(jnp.int32), start.astype(jnp.int32))
        return lax.dynamic_slice(adjoint, corner, (1, SB, WIN)).reshape(SB * WIN)

    def back_slab(carry, inputs):
        slab_blocks, slab_ids, slab_starts, slab_counts = inputs
        windows = jax.vmap(jax.vmap(cut_window))(group_grid, slab_ids, slab_starts)
        live = (slot_grid[None, :] < slab_counts[:, None]).astype(jnp.float32)
        windows = windows * live[:, :, None]
        grad_slab = jnp.einsum('gkc,gkvc->v', windows, slab_blocks.astype(jnp.float32))
        return (carry, grad_slab)
    _, backprojected = lax.scan(back_slab, jnp.zeros((), jnp.float32), (weights, block_ids, offsets, counts))
    backprojected = backprojected.reshape(NZ, PY, PX)
    image_next = image - STEP_SIZE * (backprojected + TV_WEIGHT * tv_gradient(image))
    return (image_next, residual)
```

```python
import functools

import jax
import jax.numpy as jnp
from jax import lax
from jax.experimental import pallas as pl
from jax.experimental.pallas import tpu as pltpu
from jax.sharding import PartitionSpec as P

SB = 16
WIN = 64
LANES = 128

STEP_SIZE = 0.25
TV_WEIGHT = 0.3
TV_EPS = 0.01
C1 = 8.0 / 12.0
C2 = 1.0 / 12.0
MESH = pl.DeviceIdType.MESH


def lane_iota(shape):
    return lax.broadcasted_iota(jnp.int32, shape, len(shape) - 1)


def ahead(value, shift):
    length = value.shape[-1]
    return pltpu.roll(value, (-shift) % length, value.ndim - 1)


def stencil(value):
    return C2 * ahead(value, -2) - C1 * ahead(value, -1) + C1 * ahead(value, 1) - C2 * ahead(value, 2)


def stencil_edges(value):
    length = value.shape[-1]
    at = lane_iota(value.shape)
    total = jnp.where(at >= 2, C2 * ahead(value, -2), 0.0)
    total = total - jnp.where(at >= 1, C1 * ahead(value, -1), 0.0)
    total = total + jnp.where(at < length - 1, C1 * ahead(value, 1), 0.0)
    return total - jnp.where(at < length - 2, C2 * ahead(value, 2), 0.0)


def block_mask(width):
    row = lax.broadcasted_iota(jnp.int32, (SB, width), 0)
    return lane_iota((SB, width)) // WIN == row


def gather_kernel(
    n, slots, chunks, image, weights, ids, offs, counts, measured,
    pieces_all, meas_all, meta_all, halo, wbuf,
    mine, meta, wsem, local_sem, small_send, small_recv, halo_send, halo_recv,
    meas_send, meas_recv, relay_send, piece_send, piece_recv,
):
    me = lax.axis_index("vox")
    partner = me + 1 - 2 * (me % 2)
    voxels = weights.shape[3]
    depth = voxels // chunks
    groups = mine.shape[0]
    half = n // 2

    loads = []
    for k in range(slots):
        for q in range(chunks):
            rows = pl.ds(q * depth, depth)
            load = pltpu.make_async_copy(
                weights.at[0, 0, k, rows], wbuf.at[k, rows], wsem.at[k, q]
            )
            load.start()
            loads.append(load)

    meta[...] = jnp.zeros_like(meta)
    meta[0:1, 0:slots] = ids[0]
    meta[1:2, 0:slots] = offs[0]
    barrier = pltpu.get_barrier_semaphore()
    for step in range(1, n):
        pl.semaphore_signal(barrier, inc=1, device_id={"vox": (me + step) % n}, device_id_type=MESH)
    own = [
        pltpu.make_async_copy(measured.at[0], meas_all.at[me], local_sem.at[0]),
        pltpu.make_async_copy(meta, meta_all.at[me], local_sem.at[1]),
    ]
    pl.semaphore_wait(barrier, n - 1)

    def remote(src, dst, send, recv, target):
        return pltpu.make_async_remote_copy(
            src_ref=src, dst_ref=dst, send_sem=send, recv_sem=recv,
            device_id={"vox": target}, device_id_type=MESH,
        )

    sends = []
    for step in range(1, n):
        copy = remote(meta, meta_all.at[me], small_send.at[step], small_recv.at[step], (me + step) % n)
        copy.start()
        sends.append(copy)
    for side, target in ((0, (me + 1) % n), (1, (me + n - 1) % n)):
        copy = remote(image.at[0], halo.at[side], halo_send.at[side], halo_recv.at[side], target)
        copy.start()
        sends.append(copy)
    direct = []
    for step in range(1, half):
        copy = remote(
            measured.at[0], meas_all.at[me], meas_send.at[step], meas_recv.at[step],
            (me + 2 * step) % n,
        )
        copy.start()
        direct.append(copy)
    relays = [
        remote(measured.at[0], meas_all.at[me], relay_send.at[0], meas_recv.at[half], partner)
    ]
    relays[0].start()
    for copy in own:
        copy.start()

    low = image[0].astype(jnp.bfloat16)
    flat = jnp.concatenate([low[r : r + 1] for r in range(low.shape[0])], axis=1)
    flat = jnp.broadcast_to(flat, (SB, voxels))
    mask = block_mask(SB * WIN)
    alive = counts[...]
    left = lane_iota((SB, LANES)) < WIN
    piece_copies = []
    packed = None
    for k in range(slots):
        total = jnp.zeros((SB, SB * WIN), jnp.float32)
        for q in range(chunks):
            loads[k * chunks + q].wait()
            total = total + jnp.dot(
                flat[:, q * depth : (q + 1) * depth],
                wbuf[k, q * depth : (q + 1) * depth],
                preferred_element_type=jnp.float32,
            )
        total = jnp.where(mask, total, 0.0)
        tile = total[:, 0:LANES]
        for g in range(1, SB * WIN // LANES):
            tile = tile + total[:, g * LANES : (g + 1) * LANES]
        tile = tile + pltpu.roll(tile, WIN, 1)
        tile = jnp.where(jnp.broadcast_to(alive, tile.shape) > k, tile, 0.0)
        if k % 2 == 0:
            packed = jnp.where(left, tile, 0.0)
        else:
            packed = jnp.where(left, packed, tile)
        if k % 2 == 1 or k == slots - 1:
            g = k // 2
            mine[g] = packed
            for step in range(1, n):
                copy = remote(
                    mine.at[g], pieces_all.at[me, g], piece_send.at[g, step], piece_recv.at[g, step],
                    (me + step) % n,
                )
                copy.start()
                piece_copies.append(copy)
    for g in range(groups):
        copy = pltpu.make_async_copy(mine.at[g], pieces_all.at[me, g], local_sem.at[2 + g])
        copy.start()
        own.append(copy)

    for step, copy in zip(range(1, half), direct):
        source = (me + n - 2 * step) % n
        copy.wait_recv()
        relay = remote(
            meas_all.at[source], meas_all.at[source], relay_send.at[step],
            meas_recv.at[half + step], partner,
        )
        relay.start()
        relays.append(relay)
    for copy in own:
        copy.wait()
    for copy in sends + piece_copies:
        copy.wait()
    for copy in direct:
        copy.wait_send()
    for copy in relays:
        copy.wait()


def place_kernel(
    n, slots, ids, offs, counts, wbuf, pieces_all, meas_all, meta_all, measured,
    grad, residual, signals, table, meta_sem,
):
    me = lax.axis_index("vox")
    samples = meas_all.shape[2]
    rows = meas_all.shape[1]
    count = counts[0, 0]

    tables = pltpu.make_async_copy(meta_all, table, meta_sem)
    tables.start()
    signals[...] = jnp.zeros_like(signals)
    tables.wait()
    at = lane_iota((SB, LANES))

    def place(j, carry):
        for k in range(slots):
            number = table[j, 0, k]
            start = table[j, 1, k]
            shift = start % LANES
            base = pl.multiple_of((start // LANES + 1) * LANES, LANES)
            sensors = pl.ds(pl.multiple_of(number * SB, SB), SB)
            packed = pieces_all[j, k // 2]
            if k % 2 == 1:
                packed = pltpu.roll(packed, WIN, 1)
            piece = pltpu.roll(jnp.where(at < WIN, packed, 0.0), shift, 1)
            signals[sensors, pl.ds(base, LANES)] += jnp.where(at >= shift, piece, 0.0)
            after = pl.multiple_of(base + LANES, LANES)
            signals[sensors, pl.ds(after, LANES)] += jnp.where(at < shift, piece, 0.0)
        return carry

    lax.fori_loop(0, n, place, 0)

    mask = block_mask(SB * WIN)
    at2 = lane_iota((SB, 2 * LANES))
    grad[...] = jnp.zeros_like(grad)
    for k in range(slots):

        @pl.when(k < count)
        def _():
            number = ids[0, 0, k]
            start = offs[0, 0, k]
            first = (start - 4 + LANES) // LANES
            base = pl.multiple_of(first * LANES, LANES)
            sensors = pl.ds(pl.multiple_of(number * SB, SB), SB)
            region = signals[sensors, pl.ds(base, 2 * LANES)]
            tiles = []
            for h in range(2):
                column = jnp.clip(first - 1 + h, 0, samples // LANES - 1)
                columns = pl.ds(pl.multiple_of(column * LANES, LANES), LANES)
                if rows >= SB:
                    per = rows // SB
                    lines = pl.ds(pl.multiple_of((number % per) * SB, SB), SB)
                    tiles.append(meas_all[number // per, lines, columns].astype(jnp.float32))
                else:
                    per = SB // rows
                    tiles.append(
                        jnp.concatenate(
                            [
                                meas_all[number * per + i, :, columns].astype(jnp.float32)
                                for i in range(per)
                            ],
                            axis=0,
                        )
                    )
            time = at2 + (base - LANES)
            inside = (time >= 0) & (time < samples)
            difference = jnp.where(inside, stencil(region) - jnp.concatenate(tiles, axis=1), 0.0)
            adjoint = -stencil(difference)
            begin = start + LANES - base
            turn = (2 * LANES - begin) % LANES
            first_tile = pltpu.roll(adjoint[:, 0:LANES], turn, 1)
            second_tile = pltpu.roll(adjoint[:, LANES:], turn, 1)
            window = jnp.where(at < LANES - begin, first_tile, second_tile)
            window = jnp.where(at < WIN, window, pltpu.roll(window, WIN, 1))
            spread = jnp.concatenate([window] * (SB * WIN // LANES), axis=1)
            spread = jnp.where(mask, spread, 0.0).astype(jnp.bfloat16)
            part = lax.dot_general(
                spread, wbuf[k], (((1,), (1,)), ((), ())), preferred_element_type=jnp.float32
            )
            grad[...] += jnp.sum(part, axis=0, keepdims=True)

    for r in range(0, rows, 8):
        line = pl.multiple_of((me * rows + r) // 8 * 8, 8)
        block = stencil_edges(signals[pl.ds(line, 8), pl.ds(LANES, samples)])
        if rows % 8 == 0:
            residual[0, r : r + 8] = block - measured[0, r : r + 8].astype(jnp.float32)
        else:
            part = block[0:rows]
            for i in range(1, 8 // rows):
                chosen = jnp.full(part.shape, (me * rows) % 8) == i * rows
                part = jnp.where(chosen, block[i * rows : (i + 1) * rows], part)
            residual[0] = part - measured[0].astype(jnp.float32)


def update_kernel(n, ns, grad, image, halo, out, parts, send, recv):
    mine = lax.axis_index("sen")
    place = lax.axis_index("vox")
    barrier = pltpu.get_barrier_semaphore()
    for step in range(1, ns):
        pl.semaphore_signal(
            barrier, inc=1, device_id={"sen": (mine + step) % ns}, device_id_type=MESH
        )
    pl.semaphore_wait(barrier, ns - 1)
    copies = []
    for step in range(1, ns):
        copy = pltpu.make_async_remote_copy(
            src_ref=grad, dst_ref=parts.at[mine], send_sem=send.at[step], recv_sem=recv.at[step],
            device_id={"sen": (mine + step) % ns}, device_id_type=MESH,
        )
        copy.start()
        copies.append(copy)

    def units(volume, step_z):
        shape = volume.shape
        row = lax.broadcasted_iota(jnp.int32, shape, 0)
        below = jnp.concatenate([volume[1:], volume[shape[0] - 1 :]], axis=0)
        step_y = below - volume
        step_x = jnp.where(lane_iota(shape) < shape[1] - 1, ahead(volume, 1) - volume, 0.0)
        size = jnp.sqrt(step_z * step_z + step_y * step_y + step_x * step_x + TV_EPS)
        return step_z / size, step_y / size, step_x / size, row

    volume = image[0]
    before, after = halo[0], halo[1]
    is_first = jnp.full(volume.shape, place) == 0
    is_last = jnp.full(volume.shape, place) == n - 1
    lower_z, _, _, _ = units(before, volume - before)
    unit_z, unit_y, unit_x, row = units(volume, jnp.where(is_last, 0.0, after - volume))
    tv = jnp.where(is_first, 0.0, lower_z) - unit_z
    shifted_y = jnp.concatenate([jnp.zeros_like(unit_y[0:1]), unit_y[: unit_y.shape[0] - 1]], axis=0)
    tv = tv + shifted_y - unit_y
    tv = tv + jnp.where(lane_iota(volume.shape) >= 1, ahead(unit_x, -1), 0.0) - unit_x

    for copy in copies:
        copy.wait()
    flat = None
    for index in range(ns):
        chosen = jnp.full(grad.shape, mine) == index
        term = jnp.where(chosen, grad[...], parts[index])
        flat = term if flat is None else flat + term
    width = volume.shape[1]
    for r in range(volume.shape[0]):
        total = flat[:, r * width : (r + 1) * width]
        out[0, r : r + 1] = volume[r : r + 1] - STEP_SIZE * (total + TV_WEIGHT * tv[r : r + 1])


def on_device(image, weights, block_ids, offsets, counts, measured):
    n = lax.axis_size("vox")
    ns = lax.axis_size("sen")
    slots, voxels, cells = weights.shape[2:]
    rows, samples = measured.shape[1:]
    groups = (slots + 1) // 2
    chunks = 4
    vmem = pl.BlockSpec(memory_space=pltpu.VMEM)
    smem = pl.BlockSpec(memory_space=pltpu.SMEM)
    anywhere = pl.BlockSpec(memory_space=pl.ANY)
    hbm = pl.BlockSpec(memory_space=pltpu.HBM)
    dma = pltpu.SemaphoreType.DMA
    half = n // 2
    pieces_all, meas_all, meta_all, halo, held = pl.pallas_call(
        functools.partial(gather_kernel, n, slots, chunks),
        out_shape=(
            jax.ShapeDtypeStruct((n, groups, SB, LANES), jnp.float32),
            jax.ShapeDtypeStruct((n, rows, samples), jnp.bfloat16),
            jax.ShapeDtypeStruct((n, 2, LANES), jnp.int32),
            jax.ShapeDtypeStruct((2,) + image.shape[1:], jnp.float32),
            jax.ShapeDtypeStruct((slots, voxels, cells), jnp.bfloat16),
        ),
        in_specs=[vmem, hbm, vmem, vmem, vmem, vmem],
        out_specs=(vmem, vmem, vmem, vmem, vmem),
        scratch_shapes=[
            pltpu.VMEM((groups, SB, LANES), jnp.float32),
            pltpu.VMEM((2, LANES), jnp.int32),
            dma((slots, chunks)),
            dma((2 + groups,)),
            dma((n,)),
            dma((n,)),
            dma((2,)),
            dma((2,)),
            dma((half,)),
            dma((n,)),
            dma((half,)),
            dma((groups, n)),
            dma((groups, n)),
        ],
        compiler_params=pltpu.CompilerParams(
            collective_id=0, has_side_effects=True, vmem_limit_bytes=50 << 20
        ),
        name="gather_kernel",
    )(image, weights, block_ids, offsets, counts, measured)

    grad, residual = pl.pallas_call(
        functools.partial(place_kernel, n, slots),
        out_shape=(
            jax.ShapeDtypeStruct((1, voxels), jnp.float32),
            jax.ShapeDtypeStruct(measured.shape, jnp.float32),
        ),
        in_specs=[smem, smem, smem, vmem, vmem, vmem, anywhere, vmem],
        out_specs=(vmem, vmem),
        scratch_shapes=[
            pltpu.VMEM((rows * n, samples + 3 * LANES), jnp.float32),
            pltpu.SMEM((n, 2, LANES), jnp.int32),
            dma,
        ],
        compiler_params=pltpu.CompilerParams(vmem_limit_bytes=16 << 20),
        name="place_kernel",
    )(block_ids, offsets, counts, held, pieces_all, meas_all, meta_all, measured)

    image_next = pl.pallas_call(
        functools.partial(update_kernel, n, ns),
        out_shape=jax.ShapeDtypeStruct(image.shape, jnp.float32),
        in_specs=[vmem, vmem, vmem],
        out_specs=vmem,
        scratch_shapes=[
            pltpu.VMEM((ns, 1, voxels), jnp.float32),
            dma((ns,)),
            dma((ns,)),
        ],
        compiler_params=pltpu.CompilerParams(collective_id=1, has_side_effects=True, vmem_limit_bytes=8 << 20),
        name="update_kernel",
    )(grad, image, halo)
    return (image_next, residual)


def solution(mesh):
    placed = (
        P("vox", None, None),
        P("vox", "sen", None, None, None),
        P("vox", "sen", None),
        P("vox", "sen", None),
        P("vox", "sen"),
        P("sen", "vox", None),
    )
    return jax.shard_map(
        on_device,
        mesh=mesh,
        in_specs=placed,
        out_specs=(P("vox", None, None), P("sen", "vox", None)),
        check_vma=False,
    )
```

```python
import functools

import jax
import jax.numpy as jnp
from jax import lax
from jax.experimental import pallas as pl
from jax.experimental.pallas import tpu as pltpu
from jax.sharding import PartitionSpec as P

SB = 16
WIN = 64
LANES = 128

STEP_SIZE = 0.25
TV_WEIGHT = 0.3
TV_EPS = 0.01
C1 = 8.0 / 12.0
C2 = 1.0 / 12.0
MESH = pl.DeviceIdType.MESH


def lane_iota(shape):
    return lax.broadcasted_iota(jnp.int32, shape, len(shape) - 1)


def ahead(value, shift):
    length = value.shape[-1]
    return pltpu.roll(value, (-shift) % length, value.ndim - 1)


def stencil(value):
    return C2 * ahead(value, -2) - C1 * ahead(value, -1) + C1 * ahead(value, 1) - C2 * ahead(value, 2)


def stencil_edges(value):
    length = value.shape[-1]
    at = lane_iota(value.shape)
    total = jnp.where(at >= 2, C2 * ahead(value, -2), 0.0)
    total = total - jnp.where(at >= 1, C1 * ahead(value, -1), 0.0)
    total = total + jnp.where(at < length - 1, C1 * ahead(value, 1), 0.0)
    return total - jnp.where(at < length - 2, C2 * ahead(value, 2), 0.0)


def block_mask(width):
    row = lax.broadcasted_iota(jnp.int32, (SB, width), 0)
    return lane_iota((SB, width)) // WIN == row


def gather_kernel(
    n, slots, chunks, image_in, weights, ids_in, offs_in, counts,
    pieces_all, meta_all, halo, wbuf,
    image, ids, offs, mine, meta,
    wsem, load_sem, local_sem, small_send, small_recv, halo_send, halo_recv,
    piece_send, piece_recv,
):
    me = lax.axis_index("vox")
    voxels = weights.shape[3]
    depth = voxels // chunks
    groups = mine.shape[0]

    arguments = []
    pairs = ((ids_in, ids), (offs_in, offs), (image_in, image))
    for i, (src, dst) in enumerate(pairs):
        load = pltpu.make_async_copy(src, dst, load_sem.at[i])
        load.start()
        arguments.append(load)
    loads = []
    for k in range(slots):
        for q in range(chunks):
            part = pl.ds(q * depth, depth)
            load = pltpu.make_async_copy(weights.at[0, 0, k, part], wbuf.at[k, part], wsem.at[k, q])
            load.start()
            loads.append(load)

    barrier = pltpu.get_barrier_semaphore()
    for step in range(1, n):
        pl.semaphore_signal(barrier, inc=1, device_id={"vox": (me + step) % n}, device_id_type=MESH)
    for load in arguments:
        load.wait()
    meta[...] = jnp.where(
        lane_iota(meta.shape) == slots, jnp.full(meta.shape, counts[0, 0]), 0
    )
    meta[0:1, 0:slots] = ids[0]
    meta[1:2, 0:slots] = offs[0]
    low = image[0].astype(jnp.bfloat16)
    flat = jnp.concatenate([low[r : r + 1] for r in range(low.shape[0])], axis=1)
    flat = jnp.broadcast_to(flat, (SB, voxels))
    mask = block_mask(SB * WIN)
    alive = jnp.full((SB, LANES), counts[0, 0])
    left = lane_iota((SB, LANES)) < WIN
    pl.semaphore_wait(barrier, n - 1)

    def remote(src, dst, send, recv, target):
        return pltpu.make_async_remote_copy(
            src_ref=src, dst_ref=dst, send_sem=send, recv_sem=recv,
            device_id={"vox": target}, device_id_type=MESH,
        )

    small, sends = [], []
    for step in range(1, n):
        copy = remote(meta, meta_all.at[me], small_send.at[step], small_recv.at[step], (me + step) % n)
        copy.start()
        small.append(copy)
    own_meta = pltpu.make_async_copy(meta, meta_all.at[me], local_sem.at[0])
    own_meta.start()
    for side, target in ((0, (me + 1) % n), (1, (me + n - 1) % n)):
        copy = remote(image.at[0], halo.at[side], halo_send.at[side], halo_recv.at[side], target)
        copy.start()
        sends.append(copy)

    locals_ = [own_meta]
    packed = None
    for k in range(slots):
        total = jnp.zeros((SB, SB * WIN), jnp.float32)
        for q in range(chunks):
            loads[k * chunks + q].wait()
            total = total + jnp.dot(
                flat[:, q * depth : (q + 1) * depth],
                wbuf[k, q * depth : (q + 1) * depth],
                preferred_element_type=jnp.float32,
            )
        total = jnp.where(mask, total, 0.0)
        tile = total[:, 0:LANES]
        for g in range(1, SB * WIN // LANES):
            tile = tile + total[:, g * LANES : (g + 1) * LANES]
        tile = tile + pltpu.roll(tile, WIN, 1)
        tile = jnp.where(alive > k, tile, 0.0)
        packed = jnp.where(left, tile, 0.0) if k % 2 == 0 else jnp.where(left, packed, tile)
        if k % 2 == 1 or k == slots - 1:
            g = k // 2
            mine[g] = packed
            for step in range(1, n):
                copy = remote(
                    mine.at[g], pieces_all.at[me, g], piece_send.at[g, step], piece_recv.at[g, step],
                    (me + step) % n,
                )
                copy.start()
                sends.append(copy)
            copy = pltpu.make_async_copy(mine.at[g], pieces_all.at[me, g], local_sem.at[1 + g])
            copy.start()
            locals_.append(copy)

    for copy in locals_:
        copy.wait()
    for copy in small + sends:
        copy.wait()


def place_kernel(
    n, slots, pieces_all, meta_all, measured,
    windows, residual, signals, adjoints, table, meta_sem,
):
    me = lax.axis_index("vox")
    rows, samples = measured.shape[1:]
    tables = pltpu.make_async_copy(meta_all, table, meta_sem)
    tables.start()
    signals[...] = jnp.zeros_like(signals)
    adjoints[:, pl.ds(samples, LANES)] = jnp.zeros((adjoints.shape[0], LANES), jnp.float32)
    if rows < SB:
        adjoints[...] = jnp.zeros_like(adjoints)
    tables.wait()
    at = lane_iota((SB, LANES))

    def place(j, carry):
        for k in range(slots):
            number = table[j, 0, k]
            start = table[j, 1, k]
            shift = start % LANES
            base = pl.multiple_of((start // LANES + 1) * LANES, LANES)
            sensors = pl.ds(pl.multiple_of(number * SB, SB), SB)
            packed = pieces_all[j, k // 2]
            keep = (at < WIN) if k % 2 == 0 else (at >= WIN)
            turn = shift if k % 2 == 0 else (shift + WIN) % LANES
            piece = pltpu.roll(jnp.where(keep, packed, 0.0), turn, 1)
            signals[sensors, pl.ds(base, LANES)] += jnp.where(at >= shift, piece, 0.0)
            after = pl.multiple_of(base + LANES, LANES)
            signals[sensors, pl.ds(after, LANES)] += jnp.where(at < shift, piece, 0.0)
        return carry

    lax.fori_loop(0, n, place, 0)

    for r in range(0, rows, 8):
        line = pl.multiple_of((me * rows + r) // 8 * 8, 8)
        block = stencil_edges(signals[pl.ds(line, 8), pl.ds(LANES, samples)])
        if rows % 8 == 0:
            block = block - measured[0, r : r + 8].astype(jnp.float32)
            residual[0, r : r + 8] = block
            block = -stencil_edges(block)
        else:
            which = jnp.full((rows, samples), (me * rows) % 8)
            part = block[0:rows]
            for i in range(1, 8 // rows):
                part = jnp.where(which == i * rows, block[i * rows : (i + 1) * rows], part)
            part = part - measured[0].astype(jnp.float32)
            residual[0] = part
            part = -stencil_edges(part)
            block = jnp.concatenate(
                [jnp.where(which == i * rows, part, 0.0) for i in range(8 // rows)], axis=0
            )
        spot = r if rows >= SB else pl.multiple_of((me * rows + r) % SB // 8 * 8, 8)
        adjoints[pl.ds(spot, 8), pl.ds(0, samples)] = block

    per = max(rows // SB, 1)
    home = me * rows // SB

    def cut(j, carry):
        packed = None
        for k in range(slots):
            number = table[j, 0, k]
            start = table[j, 1, k]
            near = number - home
            mine = (near >= 0) & (near < per) & (k < table[j, 0, slots])
            line = pl.ds(pl.multiple_of(jnp.clip(near, 0, per - 1) * SB, SB), SB)
            column = pl.multiple_of(start // LANES * LANES, LANES)
            shift = start % LANES
            turn = (LANES - shift + (k % 2) * WIN) % LANES
            first = pltpu.roll(adjoints[line, pl.ds(column, LANES)], turn, 1)
            second = pltpu.roll(
                adjoints[line, pl.ds(pl.multiple_of(column + LANES, LANES), LANES)], turn, 1
            )
            window = jnp.where(at - (k % 2) * WIN < LANES - shift, first, second)
            live = jnp.full(window.shape, mine.astype(jnp.int32))
            window = jnp.where(live > 0, window, 0.0)
            packed = window if k % 2 == 0 else jnp.where(at < WIN, packed, window)
            if k % 2 == 1 or k == slots - 1:
                windows[j, k // 2] = packed.astype(windows.dtype)
        return carry

    lax.fori_loop(0, n, cut, 0)


def variation(n, place, image, halo):
    def units(volume, step_z):
        shape = volume.shape
        row = lax.broadcasted_iota(jnp.int32, shape, 0)
        below = jnp.concatenate([volume[1:], volume[shape[0] - 1 :]], axis=0)
        step_y = below - volume
        step_x = jnp.where(lane_iota(shape) < shape[1] - 1, ahead(volume, 1) - volume, 0.0)
        size = jnp.sqrt(step_z * step_z + step_y * step_y + step_x * step_x + TV_EPS)
        return step_z / size, step_y / size, step_x / size, row

    volume = image[0]
    before, after = halo[0], halo[1]
    is_first = jnp.full(volume.shape, place) == 0
    is_last = jnp.full(volume.shape, place) == n - 1
    lower_z, _, _, _ = units(before, volume - before)
    unit_z, unit_y, unit_x, row = units(volume, jnp.where(is_last, 0.0, after - volume))
    tv = jnp.where(is_first, 0.0, lower_z) - unit_z
    shifted_y = jnp.concatenate([jnp.zeros_like(unit_y[0:1]), unit_y[: unit_y.shape[0] - 1]], axis=0)
    tv = tv + shifted_y - unit_y
    tv = tv + jnp.where(lane_iota(volume.shape) >= 1, ahead(unit_x, -1), 0.0) - unit_x
    return tv


def update_kernel(
    n, ns, windows, wbuf, image, halo, out, windows_all, grad, parts, send, recv, window_send, window_recv
):
    mine = lax.axis_index("sen")
    place = lax.axis_index("vox")
    barrier = pltpu.get_barrier_semaphore()
    for step in range(1, ns):
        pl.semaphore_signal(
            barrier, inc=1, device_id={"sen": (mine + step) % ns}, device_id_type=MESH
        )
    for step in range(1, n):
        pl.semaphore_signal(
            barrier, inc=1, device_id={"vox": (place + step) % n}, device_id_type=MESH
        )
    pl.semaphore_wait(barrier, ns + n - 2)
    exchanges = []
    for step in range(1, n):
        to = (place + step) % n
        copy = pltpu.make_async_remote_copy(
            src_ref=windows.at[to], dst_ref=windows_all.at[step - 1], send_sem=window_send.at[step],
            recv_sem=window_recv.at[step], device_id={"vox": to}, device_id_type=MESH,
        )
        copy.start()
        exchanges.append(copy)
    tv = variation(n, place, image, halo)
    for copy in exchanges:
        copy.wait()
    mask = block_mask(SB * WIN)
    left = lane_iota((SB, LANES)) < WIN
    part = None
    for g in range(windows.shape[1]):
        packed = windows[place, g].astype(jnp.float32)
        for step in range(1, n):
            packed = packed + windows_all[step - 1, g].astype(jnp.float32)
        turned = pltpu.roll(packed, WIN, 1)
        for k in range(2 * g, min(2 * g + 2, wbuf.shape[0])):
            window = jnp.where(left, packed, turned) if k % 2 == 0 else jnp.where(left, turned, packed)
            spread = jnp.concatenate([window] * (SB * WIN // LANES), axis=1)
            spread = jnp.where(mask, spread, 0.0).astype(jnp.bfloat16)
            term = lax.dot_general(
                spread, wbuf[k], (((1,), (1,)), ((), ())), preferred_element_type=jnp.float32
            )
            part = term if part is None else part + term
    grad[...] = jnp.sum(part, axis=0, keepdims=True)
    copies = []
    for step in range(1, ns):
        copy = pltpu.make_async_remote_copy(
            src_ref=grad, dst_ref=parts.at[mine], send_sem=send.at[step], recv_sem=recv.at[step],
            device_id={"sen": (mine + step) % ns}, device_id_type=MESH,
        )
        copy.start()
        copies.append(copy)

    for copy in copies:
        copy.wait()
    flat = None
    for index in range(ns):
        chosen = jnp.full(grad.shape, mine) == index
        term = jnp.where(chosen, grad[...], parts[index])
        flat = term if flat is None else flat + term
    volume = image[0]
    width = volume.shape[1]
    for r in range(volume.shape[0]):
        total = flat[:, r * width : (r + 1) * width]
        out[0, r : r + 1] = volume[r : r + 1] - STEP_SIZE * (total + TV_WEIGHT * tv[r : r + 1])


def on_device(image, weights, block_ids, offsets, counts, measured):
    n = lax.axis_size("vox")
    ns = lax.axis_size("sen")
    slots, voxels, cells = weights.shape[2:]
    rows, samples = measured.shape[1:]
    groups = (slots + 1) // 2
    chunks = 4
    vmem = pl.BlockSpec(memory_space=pltpu.VMEM)
    smem = pl.BlockSpec(memory_space=pltpu.SMEM)
    hbm = pl.BlockSpec(memory_space=pltpu.HBM)
    anywhere = pl.BlockSpec(memory_space=pl.ANY)
    dma = pltpu.SemaphoreType.DMA
    shape = jax.ShapeDtypeStruct

    def pin(value):
        return pltpu.with_memory_space_constraint(value, pltpu.HBM)

    pieces_all, meta_all, halo, held = pl.pallas_call(
        functools.partial(gather_kernel, n, slots, chunks),
        out_shape=(
            shape((n, groups, SB, LANES), jnp.float32),
            shape((n, 2, LANES), jnp.int32),
            shape((2,) + image.shape[1:], jnp.float32),
            shape((slots, voxels, cells), jnp.bfloat16),
        ),
        in_specs=[hbm, hbm, hbm, hbm, smem],
        out_specs=(vmem,) * 4,
        scratch_shapes=[
            pltpu.VMEM(image.shape, jnp.float32),
            pltpu.VMEM(block_ids.shape, jnp.int32),
            pltpu.VMEM(offsets.shape, jnp.int32),
            pltpu.VMEM((groups, SB, LANES), jnp.float32),
            pltpu.VMEM((2, LANES), jnp.int32),
            dma((slots, chunks)),
            dma((3,)),
            dma((1 + groups,)),
            dma((n,)),
            dma((n,)),
            dma((2,)),
            dma((2,)),
            dma((groups, n)),
            dma((groups, n)),
        ],
        compiler_params=pltpu.CompilerParams(
            collective_id=0, has_side_effects=True, vmem_limit_bytes=16 << 20
        ),
        name="gather_kernel",
    )(pin(image), pin(weights), pin(block_ids), pin(offsets), counts)

    windows, residual = pl.pallas_call(
        functools.partial(place_kernel, n, slots),
        out_shape=(
            shape((n, groups, SB, LANES), jnp.bfloat16),
            shape(measured.shape, jnp.float32),
        ),
        in_specs=[vmem, anywhere, vmem],
        out_specs=(vmem, vmem),
        scratch_shapes=[
            pltpu.VMEM((rows * n, samples + 3 * LANES), jnp.float32),
            pltpu.VMEM((max(rows, SB), samples + LANES), jnp.float32),
            pltpu.SMEM((n, 2, LANES), jnp.int32),
            dma,
        ],
        compiler_params=pltpu.CompilerParams(vmem_limit_bytes=16 << 20),
        name="place_kernel",
    )(pieces_all, meta_all, measured)

    image_next = pl.pallas_call(
        functools.partial(update_kernel, n, ns),
        out_shape=shape(image.shape, jnp.float32),
        in_specs=[vmem] * 4,
        out_specs=vmem,
        scratch_shapes=[
            pltpu.VMEM((n - 1, groups, SB, LANES), jnp.bfloat16),
            pltpu.VMEM((1, voxels), jnp.float32),
            pltpu.VMEM((ns, 1, voxels), jnp.float32),
            dma((ns,)),
            dma((ns,)),
            dma((n,)),
            dma((n,)),
        ],
        compiler_params=pltpu.CompilerParams(
            collective_id=1, has_side_effects=True, vmem_limit_bytes=16 << 20
        ),
        name="update_kernel",
    )(windows, held, image, halo)
    return (image_next, residual)


def solution(mesh):
    placed = (
        P("vox", None, None),
        P("vox", "sen", None, None, None),
        P("vox", "sen", None),
        P("vox", "sen", None),
        P("vox", "sen"),
        P("sen", "vox", None),
    )
    return jax.shard_map(
        on_device,
        mesh=mesh,
        in_specs=placed,
        out_specs=(P("vox", None, None), P("sen", "vox", None)),
        check_vma=False,
    )
```

```python
import functools

import jax
import jax.numpy as jnp
from jax import lax
from jax.experimental import pallas as pl
from jax.experimental.pallas import tpu as pltpu
from jax.sharding import PartitionSpec as P

SB = 16
WIN = 64
LANES = 128

STEP_SIZE = 0.25
TV_WEIGHT = 0.3
TV_EPS = 0.01
C1 = 8.0 / 12.0
C2 = 1.0 / 12.0
MESH = pl.DeviceIdType.MESH


def lane_iota(shape):
    return lax.broadcasted_iota(jnp.int32, shape, len(shape) - 1)


def ahead(value, shift):
    length = value.shape[-1]
    return pltpu.roll(value, (-shift) % length, value.ndim - 1)


def stencil(value):
    return C2 * ahead(value, -2) - C1 * ahead(value, -1) + C1 * ahead(value, 1) - C2 * ahead(value, 2)


def stencil_edges(value):
    length = value.shape[-1]
    at = lane_iota(value.shape)
    total = jnp.where(at >= 2, C2 * ahead(value, -2), 0.0)
    total = total - jnp.where(at >= 1, C1 * ahead(value, -1), 0.0)
    total = total + jnp.where(at < length - 1, C1 * ahead(value, 1), 0.0)
    return total - jnp.where(at < length - 2, C2 * ahead(value, 2), 0.0)


def block_mask(width):
    row = lax.broadcasted_iota(jnp.int32, (SB, width), 0)
    return lane_iota((SB, width)) // WIN == row


def gather_kernel(
    n, slots, chunks, image_in, weights, ids_in, offs_in, counts,
    pieces_all, meta_all, halo, wbuf,
    image, ids, offs, mine, meta,
    wsem, load_sem, local_sem, small_send, small_recv, halo_send, halo_recv,
    piece_send, piece_recv,
):
    me = lax.axis_index("vox")
    voxels = weights.shape[3]
    depth = voxels // chunks
    groups = mine.shape[0]

    arguments = []
    pairs = ((ids_in, ids), (offs_in, offs), (image_in, image))
    for i, (src, dst) in enumerate(pairs):
        load = pltpu.make_async_copy(src, dst, load_sem.at[i])
        load.start()
        arguments.append(load)
    loads = []
    for k in range(slots):
        for q in range(chunks):
            part = pl.ds(q * depth, depth)
            load = pltpu.make_async_copy(weights.at[0, 0, k, part], wbuf.at[k, part], wsem.at[k, q])
            load.start()
            loads.append(load)

    barrier = pltpu.get_barrier_semaphore()
    for step in range(1, n):
        pl.semaphore_signal(barrier, inc=1, device_id={"vox": (me + step) % n}, device_id_type=MESH)
    for load in arguments:
        load.wait()
    meta[...] = jnp.where(
        lane_iota(meta.shape) == slots, jnp.full(meta.shape, counts[0, 0]), 0
    )
    meta[0:1, 0:slots] = ids[0]
    meta[1:2, 0:slots] = offs[0]
    low = image[0].astype(jnp.bfloat16)
    flat = jnp.concatenate([low[r : r + 1] for r in range(low.shape[0])], axis=1)
    flat = jnp.broadcast_to(flat, (SB, voxels))
    mask = block_mask(SB * WIN)
    alive = jnp.full((SB, LANES), counts[0, 0])
    left = lane_iota((SB, LANES)) < WIN
    def remote(src, dst, send, recv, target):
        return pltpu.make_async_remote_copy(
            src_ref=src, dst_ref=dst, send_sem=send, recv_sem=recv,
            device_id={"vox": target}, device_id_type=MESH,
        )

    small, sends, locals_ = [], [], []

    def greet():
        pl.semaphore_wait(barrier, n - 1)
        for step in range(1, n):
            copy = remote(meta, meta_all.at[me], small_send.at[step], small_recv.at[step], (me + step) % n)
            copy.start()
            small.append(copy)
        own_meta = pltpu.make_async_copy(meta, meta_all.at[me], local_sem.at[0])
        own_meta.start()
        locals_.append(own_meta)
        for side, target in ((0, (me + 1) % n), (1, (me + n - 1) % n)):
            copy = remote(image.at[0], halo.at[side], halo_send.at[side], halo_recv.at[side], target)
            copy.start()
            sends.append(copy)

    packed = None
    for k in range(slots):
        total = jnp.zeros((SB, SB * WIN), jnp.float32)
        for q in range(chunks):
            loads[k * chunks + q].wait()
            total = total + jnp.dot(
                flat[:, q * depth : (q + 1) * depth],
                wbuf[k, q * depth : (q + 1) * depth],
                preferred_element_type=jnp.float32,
            )
        total = jnp.where(mask, total, 0.0)
        tile = total[:, 0:LANES]
        for g in range(1, SB * WIN // LANES):
            tile = tile + total[:, g * LANES : (g + 1) * LANES]
        tile = tile + pltpu.roll(tile, WIN, 1)
        tile = jnp.where(alive > k, tile, 0.0)
        packed = jnp.where(left, tile, 0.0) if k % 2 == 0 else jnp.where(left, packed, tile)
        if k % 2 == 1 or k == slots - 1:
            g = k // 2
            mine[g] = packed
            if g == 0:
                greet()
            for step in range(1, n):
                copy = remote(
                    mine.at[g], pieces_all.at[me, g], piece_send.at[g, step], piece_recv.at[g, step],
                    (me + step) % n,
                )
                copy.start()
                sends.append(copy)
            copy = pltpu.make_async_copy(mine.at[g], pieces_all.at[me, g], local_sem.at[1 + g])
            copy.start()
            locals_.append(copy)

    for copy in locals_:
        copy.wait()
    for copy in small + sends:
        copy.wait()


def place_kernel(
    n, slots, pieces_all, meta_all, measured,
    windows, residual, signals, adjoints, table, meta_sem,
):
    me = lax.axis_index("vox")
    rows, samples = measured.shape[1:]
    tables = pltpu.make_async_copy(meta_all, table, meta_sem)
    tables.start()
    signals[...] = jnp.zeros_like(signals)
    adjoints[:, pl.ds(samples, LANES)] = jnp.zeros((adjoints.shape[0], LANES), jnp.float32)
    if rows < SB:
        adjoints[...] = jnp.zeros_like(adjoints)
    tables.wait()
    at = lane_iota((SB, LANES))

    per = max(rows // SB, 1)
    home = me * rows // SB

    def place(j, carry):
        for k in range(slots):
            near = table[j, 0, k] - home
            number = jnp.where((near >= 0) & (near < per), near, per)
            start = table[j, 1, k]
            shift = start % LANES
            base = pl.multiple_of((start // LANES + 1) * LANES, LANES)
            sensors = pl.ds(pl.multiple_of(number * SB, SB), SB)
            packed = pieces_all[j, k // 2]
            keep = (at < WIN) if k % 2 == 0 else (at >= WIN)
            turn = shift if k % 2 == 0 else (shift + WIN) % LANES
            piece = pltpu.roll(jnp.where(keep, packed, 0.0), turn, 1)
            signals[sensors, pl.ds(base, LANES)] += jnp.where(at >= shift, piece, 0.0)
            after = pl.multiple_of(base + LANES, LANES)
            signals[sensors, pl.ds(after, LANES)] += jnp.where(at < shift, piece, 0.0)
        return carry

    lax.fori_loop(0, n, place, 0)

    for r in range(0, rows, 8):
        line = pl.multiple_of((me * rows + r) // 8 * 8, 8)
        near = pl.multiple_of(line - home * SB, 8)
        block = stencil_edges(signals[pl.ds(near, 8), pl.ds(LANES, samples)])
        if rows % 8 == 0:
            block = block - measured[0, r : r + 8].astype(jnp.float32)
            residual[0, r : r + 8] = block
            block = -stencil_edges(block)
        else:
            which = jnp.full((rows, samples), (me * rows) % 8)
            part = block[0:rows]
            for i in range(1, 8 // rows):
                part = jnp.where(which == i * rows, block[i * rows : (i + 1) * rows], part)
            part = part - measured[0].astype(jnp.float32)
            residual[0] = part
            part = -stencil_edges(part)
            block = jnp.concatenate(
                [jnp.where(which == i * rows, part, 0.0) for i in range(8 // rows)], axis=0
            )
        spot = r if rows >= SB else pl.multiple_of((me * rows + r) % SB // 8 * 8, 8)
        adjoints[pl.ds(spot, 8), pl.ds(0, samples)] = block

    def cut(j, carry):
        packed = None
        for k in range(slots):
            number = table[j, 0, k]
            start = table[j, 1, k]
            near = number - home
            mine = (near >= 0) & (near < per) & (k < table[j, 0, slots])
            line = pl.ds(pl.multiple_of(jnp.clip(near, 0, per - 1) * SB, SB), SB)
            column = pl.multiple_of(start // LANES * LANES, LANES)
            shift = start % LANES
            turn = (LANES - shift + (k % 2) * WIN) % LANES
            first = pltpu.roll(adjoints[line, pl.ds(column, LANES)], turn, 1)
            second = pltpu.roll(
                adjoints[line, pl.ds(pl.multiple_of(column + LANES, LANES), LANES)], turn, 1
            )
            window = jnp.where(at - (k % 2) * WIN < LANES - shift, first, second)
            live = jnp.full(window.shape, mine.astype(jnp.int32))
            window = jnp.where(live > 0, window, 0.0)
            packed = window if k % 2 == 0 else jnp.where(at < WIN, packed, window)
            if k % 2 == 1 or k == slots - 1:
                windows[j, k // 2] = packed.astype(windows.dtype)
        return carry

    lax.fori_loop(0, n, cut, 0)


def variation(n, place, image, halo):
    def units(volume, step_z):
        shape = volume.shape
        row = lax.broadcasted_iota(jnp.int32, shape, 0)
        below = jnp.concatenate([volume[1:], volume[shape[0] - 1 :]], axis=0)
        step_y = below - volume
        step_x = jnp.where(lane_iota(shape) < shape[1] - 1, ahead(volume, 1) - volume, 0.0)
        size = jnp.sqrt(step_z * step_z + step_y * step_y + step_x * step_x + TV_EPS)
        return step_z / size, step_y / size, step_x / size, row

    volume = image[0]
    before, after = halo[0], halo[1]
    is_first = jnp.full(volume.shape, place) == 0
    is_last = jnp.full(volume.shape, place) == n - 1
    lower_z, _, _, _ = units(before, volume - before)
    unit_z, unit_y, unit_x, row = units(volume, jnp.where(is_last, 0.0, after - volume))
    tv = jnp.where(is_first, 0.0, lower_z) - unit_z
    shifted_y = jnp.concatenate([jnp.zeros_like(unit_y[0:1]), unit_y[: unit_y.shape[0] - 1]], axis=0)
    tv = tv + shifted_y - unit_y
    tv = tv + jnp.where(lane_iota(volume.shape) >= 1, ahead(unit_x, -1), 0.0) - unit_x
    return tv


def update_kernel(
    n, ns, windows, wbuf, image, halo, out, windows_all, grad, parts, send, recv, window_send, window_recv
):
    mine = lax.axis_index("sen")
    place = lax.axis_index("vox")
    barrier = pltpu.get_barrier_semaphore()
    for step in range(1, ns):
        pl.semaphore_signal(
            barrier, inc=1, device_id={"sen": (mine + step) % ns}, device_id_type=MESH
        )
    for step in range(1, n):
        pl.semaphore_signal(
            barrier, inc=1, device_id={"vox": (place + step) % n}, device_id_type=MESH
        )
    pl.semaphore_wait(barrier, ns + n - 2)
    exchanges = []
    for step in range(1, n):
        to = (place + step) % n
        copy = pltpu.make_async_remote_copy(
            src_ref=windows.at[to], dst_ref=windows_all.at[step - 1], send_sem=window_send.at[step],
            recv_sem=window_recv.at[step], device_id={"vox": to}, device_id_type=MESH,
        )
        copy.start()
        exchanges.append(copy)
    tv = variation(n, place, image, halo)
    for copy in exchanges:
        copy.wait()
    mask = block_mask(SB * WIN)
    left = lane_iota((SB, LANES)) < WIN
    part = None
    for g in range(windows.shape[1]):
        packed = windows[place, g].astype(jnp.float32)
        for step in range(1, n):
            packed = packed + windows_all[step - 1, g].astype(jnp.float32)
        turned = pltpu.roll(packed, WIN, 1)
        for k in range(2 * g, min(2 * g + 2, wbuf.shape[0])):
            window = jnp.where(left, packed, turned) if k % 2 == 0 else jnp.where(left, turned, packed)
            spread = jnp.concatenate([window] * (SB * WIN // LANES), axis=1)
            spread = jnp.where(mask, spread, 0.0).astype(jnp.bfloat16)
            term = lax.dot_general(
                spread, wbuf[k], (((1,), (1,)), ((), ())), preferred_element_type=jnp.float32
            )
            part = term if part is None else part + term
    grad[...] = jnp.sum(part, axis=0, keepdims=True)
    copies = []
    for step in range(1, ns):
        copy = pltpu.make_async_remote_copy(
            src_ref=grad, dst_ref=parts.at[mine], send_sem=send.at[step], recv_sem=recv.at[step],
            device_id={"sen": (mine + step) % ns}, device_id_type=MESH,
        )
        copy.start()
        copies.append(copy)

    for copy in copies:
        copy.wait()
    flat = None
    for index in range(ns):
        chosen = jnp.full(grad.shape, mine) == index
        term = jnp.where(chosen, grad[...], parts[index])
        flat = term if flat is None else flat + term
    volume = image[0]
    width = volume.shape[1]
    for r in range(volume.shape[0]):
        total = flat[:, r * width : (r + 1) * width]
        out[0, r : r + 1] = volume[r : r + 1] - STEP_SIZE * (total + TV_WEIGHT * tv[r : r + 1])


def on_device(image, weights, block_ids, offsets, counts, measured):
    n = lax.axis_size("vox")
    ns = lax.axis_size("sen")
    slots, voxels, cells = weights.shape[2:]
    rows, samples = measured.shape[1:]
    groups = (slots + 1) // 2
    chunks = 4
    vmem = pl.BlockSpec(memory_space=pltpu.VMEM)
    smem = pl.BlockSpec(memory_space=pltpu.SMEM)
    hbm = pl.BlockSpec(memory_space=pltpu.HBM)
    anywhere = pl.BlockSpec(memory_space=pl.ANY)
    dma = pltpu.SemaphoreType.DMA
    shape = jax.ShapeDtypeStruct

    def pin(value):
        return pltpu.with_memory_space_constraint(value, pltpu.HBM)

    pieces_all, meta_all, halo, held = pl.pallas_call(
        functools.partial(gather_kernel, n, slots, chunks),
        out_shape=(
            shape((n, groups, SB, LANES), jnp.float32),
            shape((n, 2, LANES), jnp.int32),
            shape((2,) + image.shape[1:], jnp.float32),
            shape((slots, voxels, cells), jnp.bfloat16),
        ),
        in_specs=[hbm, hbm, hbm, hbm, smem],
        out_specs=(vmem,) * 4,
        scratch_shapes=[
            pltpu.VMEM(image.shape, jnp.float32),
            pltpu.VMEM(block_ids.shape, jnp.int32),
            pltpu.VMEM(offsets.shape, jnp.int32),
            pltpu.VMEM((groups, SB, LANES), jnp.float32),
            pltpu.VMEM((2, LANES), jnp.int32),
            dma((slots, chunks)),
            dma((3,)),
            dma((1 + groups,)),
            dma((n,)),
            dma((n,)),
            dma((2,)),
            dma((2,)),
            dma((groups, n)),
            dma((groups, n)),
        ],
        compiler_params=pltpu.CompilerParams(
            collective_id=0, has_side_effects=True, vmem_limit_bytes=16 << 20
        ),
        name="gather_kernel",
    )(pin(image), pin(weights), pin(block_ids), pin(offsets), counts)

    windows, residual = pl.pallas_call(
        functools.partial(place_kernel, n, slots),
        out_shape=(
            shape((n, groups, SB, LANES), jnp.bfloat16),
            shape(measured.shape, jnp.float32),
        ),
        in_specs=[vmem, anywhere, vmem],
        out_specs=(vmem, vmem),
        scratch_shapes=[
            pltpu.VMEM((max(rows, SB) + SB, samples + 3 * LANES), jnp.float32),
            pltpu.VMEM((max(rows, SB), samples + LANES), jnp.float32),
            pltpu.SMEM((n, 2, LANES), jnp.int32),
            dma,
        ],
        compiler_params=pltpu.CompilerParams(vmem_limit_bytes=16 << 20),
        name="place_kernel",
    )(pieces_all, meta_all, measured)

    image_next = pl.pallas_call(
        functools.partial(update_kernel, n, ns),
        out_shape=shape(image.shape, jnp.float32),
        in_specs=[vmem] * 4,
        out_specs=vmem,
        scratch_shapes=[
            pltpu.VMEM((n - 1, groups, SB, LANES), jnp.bfloat16),
            pltpu.VMEM((1, voxels), jnp.float32),
            pltpu.VMEM((ns, 1, voxels), jnp.float32),
            dma((ns,)),
            dma((ns,)),
            dma((n,)),
            dma((n,)),
        ],
        compiler_params=pltpu.CompilerParams(
            collective_id=1, has_side_effects=True, vmem_limit_bytes=16 << 20
        ),
        name="update_kernel",
    )(windows, held, image, halo)
    return (image_next, residual)


def solution(mesh):
    placed = (
        P("vox", None, None),
        P("vox", "sen", None, None, None),
        P("vox", "sen", None),
        P("vox", "sen", None),
        P("vox", "sen"),
        P("sen", "vox", None),
    )
    return jax.shard_map(
        on_device,
        mesh=mesh,
        in_specs=placed,
        out_specs=(P("vox", None, None), P("sen", "vox", None)),
        check_vma=False,
    )
```
